256 devices in a mesh: gx: 4 (over y_hi, core), gy: 8 (over z), gz: 8 (over x, y_lo).
Axes of the slice: x: 4, y: 4 (y_hi: 2, y_lo: 2; y = y_hi * 2 + y_lo), z: 8, core: 2. Of those that a mesh axis runs over, the one named last changes fastest.
Arguments:
- w_minus: bfloat16 [4, 8, 8, 3, 512, 1024], P('gx', 'gy', 'gz'), may hold values from -0.25 to 0.25
- w_plus: bfloat16 [4, 8, 8, 3, 512, 1024], P('gx', 'gy', 'gz'), may hold values from -0.25 to 0.25
- interior: bfloat16 [4, 8, 8, 512, 512], P('gx', 'gy', 'gz')
- b_minus: bfloat16 [4, 8, 8, 3, 1024], P('gx', 'gy', 'gz'), may hold values from 2 to 4
- b_plus: bfloat16 [4, 8, 8, 3, 1024], P('gx', 'gy', 'gz'), may hold values from 2 to 4
- walls: int32 [4, 8, 8, 3], P('gx', 'gy', 'gz'), may hold values from 0 to 1, as said below
Outputs:
- assembled: bfloat16 [4, 8, 8, 3, 1024, 1024], P('gx', 'gy', 'gz')
The draws below stay inside these ranges and needn't reach their ends.
Inputs may be any that keep to these rules, and one draw needn't show every extreme that they name: Every subdomain with the last index along axis a has walls 1 for axis a.
All inputs are finite; a program needn't handle non-finite values.
Results may differ from the reference program's by a relative error of at most 0.0039.
Values may be sent and summed in bfloat16 or wider, within the bound.
A program may use at most 128 MiB of HBM per device.

```python
import jax
import jax.numpy as jnp
from jax import lax

FSIDE = 32
F = 1024
R = 512
NDX = 4
NDY = 8
NDZ = 8


def draw_walls(key, part):
    shape = (NDX, NDY, NDZ, 3)
    raw = jax.random.randint(key, shape, 0, 4)
    flags = (raw == 0).astype(jnp.int32)
    which = lax.broadcasted_iota(jnp.int32, shape, 3)
    at_end = (which == 0) & (lax.broadcasted_iota(jnp.int32, shape, 0) == NDX - 1) | (which == 1) & (lax.broadcasted_iota(jnp.int32, shape, 1) == NDY - 1) | (which == 2) & (lax.broadcasted_iota(jnp.int32, shape, 2) == NDZ - 1)
    return jnp.where(at_end, 1, flags).astype(jnp.int32)


def draw_interior(key, part):
    first = jax.random.fold_in(key, 11)
    second = jax.random.fold_in(key, 12)
    shape = (NDX, NDY, NDZ, R, R)
    spread = jax.random.normal(first, shape, jnp.float32) * (0.5 / R ** 0.5)
    levels = jax.random.uniform(second, (NDX, NDY, NDZ, R), jnp.float32, 0.5, 1.5)
    eye_mask = (lax.broadcasted_iota(jnp.int32, shape, 3) == lax.broadcasted_iota(jnp.int32, shape, 4)).astype(jnp.float32)
    return (spread + eye_mask * levels[..., None]).astype(jnp.bfloat16)


def block_scale(own_key, dims, split, least, top_value):
    def one(dim, parts):
        draws = jax.random.uniform(jax.random.fold_in(jax.random.fold_in(own_key, 6), dim), (parts,), jnp.float32, least / len(split), top_value / len(split))
        return jnp.repeat(jnp.exp(draws), dims[dim] // parts).reshape((-1,) + (1,) * (len(dims) - dim - 1))

    factor_of = one(*split[0])
    for cut in split[1:]:
        factor_of = factor_of * one(*cut)
    return factor_of


def scatter_about(stream_key, shape, scale, bound, shards=(), kind=jnp.bfloat16):
    array = scale * jax.random.normal(stream_key, shape, jnp.float32)
    if shards:
        array = array * block_scale(stream_key, shape, shards, -0.22, 0.18)
    return jnp.clip(array, -bound, bound).astype(kind)


def setup_inputs(seed: int = 0) -> dict:
    splits = jax.random.split(jax.random.key(seed), 7)
    w_minus = scatter_about(splits[0], (NDX, NDY, NDZ, 3, R, F), R ** -0.5, 0.25, ((0, 4), (1, 8), (2, 8)))
    w_plus = scatter_about(splits[1], (NDX, NDY, NDZ, 3, R, F), R ** -0.5, 0.25, ((0, 4), (1, 8), (2, 8)))
    interior = draw_interior(jax.random.fold_in(splits[6], 71), 0)
    b_minus = jnp.clip(2.0 + 2.0 * jax.random.uniform(splits[3], (NDX, NDY, NDZ, 3, F), jnp.float32) ** block_scale(splits[3], (NDX, NDY, NDZ, 3, F), ((0, 4), (1, 8), (2, 8)), -0.2, 0.2), 2.0, 4.0).astype(jnp.bfloat16)
    b_plus = jnp.clip(2.0 + 2.0 * jax.random.uniform(splits[4], (NDX, NDY, NDZ, 3, F), jnp.float32) ** block_scale(splits[4], (NDX, NDY, NDZ, 3, F), ((0, 4), (1, 8), (2, 8)), -0.2, 0.2), 2.0, 4.0).astype(jnp.bfloat16)
    walls = draw_walls(jax.random.fold_in(splits[6], 71), 0)
    return {"w_minus": w_minus, "w_plus": w_plus, "interior": interior, "b_minus": b_minus, "b_plus": b_plus, "walls": walls}


def face_links():
    cells = jnp.arange(F, dtype=jnp.int32)
    rows_u = cells // FSIDE
    rows_v = cells % FSIDE
    apart = jnp.abs(rows_u[:, None] - rows_u[None, :]) + jnp.abs(rows_v[:, None] - rows_v[None, :])
    return (apart == 1).astype(jnp.float32)


def schur_block(factor, inverse, diag_part, links):
    mapped = jnp.dot(inverse, factor, preferred_element_type=jnp.float32).astype(jnp.bfloat16)
    gram = jnp.dot(factor.T, mapped, preferred_element_type=jnp.float32)
    return jnp.diag(diag_part.astype(jnp.float32)) - 0.25 * links - gram


def reference(w_minus, w_plus, interior, b_minus, b_plus, walls):
    links = face_links()

    def one_device(index):
        i = index // (NDY * NDZ)
        j = (index // NDZ) % NDY
        k = index % NDZ
        higher = [(jnp.minimum(i + 1, NDX - 1), j, k), (i, jnp.minimum(j + 1, NDY - 1), k), (i, j, jnp.minimum(k + 1, NDZ - 1))]
        blocks = []
        for axis_id in range(3):
            own = schur_block(w_plus[i, j, k, axis_id], interior[i, j, k], b_plus[i, j, k, axis_id], links)
            ni, nj, nk = higher[axis_id]
            other = schur_block(w_minus[ni, nj, nk, axis_id], interior[ni, nj, nk], b_minus[ni, nj, nk, axis_id], links)
            opened = walls[i, j, k, axis_id] == 0
            total = own + jnp.where(opened, other, jnp.zeros_like(other))
            blocks.append(total.astype(jnp.bfloat16))
        return jnp.stack(blocks)

    result = lax.map(one_device, jnp.arange(NDX * NDY * NDZ, dtype=jnp.int32))
    return result.reshape(NDX, NDY, NDZ, 3, F, F)
```

```python
import jax
import jax.numpy as jnp
from jax import lax
from jax.experimental import pallas as pl
from jax.experimental.pallas import tpu as pltpu
from jax.sharding import PartitionSpec as P

FSIDE = 32
MESH = pl.DeviceIdType.MESH
PIECES = 4


def coordinates():
    gx, gy, gz = lax.axis_index("gx"), lax.axis_index("gy"), lax.axis_index("gz")
    return gz // 2, (gx // 2) * 2 + gz % 2, gy, gx % 2


def device_at(x, y, z, c):
    return ((y // 2) * 2 + c, z, x * 2 + y % 2)


def as_int(flag):
    return jnp.where(flag, 1, 0)


def kernel(
    wm_ref, wp_ref, a_ref, bm_ref, bp_ref, walls_ref, out_ref,
    wv, av, bv, bpv, walls, acc, mapped, turned, relay_a, relay_w,
    load_sem, send_sem, recv_sem, relay_send, relay_recv, forward_send,
):
    x, y, z, c = coordinates()
    rank, width = wm_ref.shape[1], wm_ref.shape[2]
    step = width // PIECES
    odd = y % 2 == 1
    even = y % 2 == 0
    low, high = y < 2, y >= 2
    c0, c1 = c == 0, c == 1

    def cols(n):
        return pl.ds(n * step, step)

    loads = [pltpu.make_async_copy(walls_ref, walls, load_sem.at[5])]
    loads.append(pltpu.make_async_copy(bp_ref, bpv, load_sem.at[4]))
    loads.append(pltpu.make_async_copy(a_ref, av.at[0], load_sem.at[3]))
    for axis in range(3):
        loads.append(pltpu.make_async_copy(wp_ref.at[axis], wv.at[axis], load_sem.at[axis]))

    has_y = z < 7
    has_z = jnp.logical_not(odd & (x == 3))
    has_x = c0 | low
    diag = even & (x >= 1)
    diag_in = odd & (x <= 2)
    relay_in = odd & ((x >= 1) | (c0 & high))
    relay_out = even & ((x >= 1) | (c0 & high))

    barrier = pltpu.get_barrier_semaphore()

    def greet(flag, *who):
        @pl.when(flag)
        def _():
            pl.semaphore_signal(barrier, inc=1, device_id=device_at(*who), device_id_type=MESH)

    greet(has_y, x, y, z + 1, c)
    greet(even, x, y + 1, z, c)
    greet(diag_in, x + 1, y - 1, z, c)
    greet(diag_in, x + 1, y, z, c)
    greet(relay_in, x, y - 1, z, c)
    greet(c0, x, y, z, 1)
    greet(c1 & low, x, y + 2, z, 0)
    greet(c1 & low, x, 1 - y, z, 0)
    greet(c1 & low, x, 3 - y, z, 0)
    greet(c0 & low, x, 3 - y, z, 0)

    for load in loads:
        load.start()

    partners = (
        as_int(z >= 1) + as_int(odd) + as_int(diag) + as_int(odd & (x >= 1)) + as_int(relay_out)
        + as_int(c1) + as_int(c0 & high) * 2 + as_int(c0)
    )
    pl.semaphore_wait(barrier, partners)

    def source(axis, part):
        if part == 0:
            return a_ref
        if part == 5:
            return bm_ref
        return wm_ref.at[axis, :, cols(part - 1)]

    def landing(axis, part):
        if part == 0:
            return av.at[1 + axis]
        if part == 5:
            return bv.at[axis]
        return wv.at[3 + axis, :, cols(part - 1)]

    def direct(axis, part, who):
        return pltpu.make_async_remote_copy(
            source(axis, part), landing(axis, part),
            send_sem.at[axis, part], recv_sem.at[axis, part],
            device_id=device_at(*who), device_id_type=MESH,
        )

    def to_relay(axis, part, slot, who):
        target = relay_a if part == 0 else relay_w.at[slot]
        return pltpu.make_async_remote_copy(
            source(axis, part), target,
            relay_send.at[axis, slot], relay_recv.at[axis, slot],
            device_id=device_at(*who), device_id_type=MESH,
        )

    def forward(axis, part, origin, slot, who):
        return pltpu.make_async_remote_copy(
            origin, landing(axis, part),
            forward_send.at[axis, slot], recv_sem.at[axis, part],
            device_id=device_at(*who), device_id_type=MESH,
        )

    y_to = (x, y, z - 1, c)
    z_to_even = (x, y - 1, z, c)
    z_to_odd = (x - 1, y + 1, z, c)
    side = (x, y + 1, z, c)
    x_near = (x, y, z, 0)
    x_far = (x, y - 2, z, 1)
    x_relay = (x, 3 - y, z, 0)

    sent = []

    def send(flag, copy):
        @pl.when(flag)
        def _():
            copy.start()

        sent.append((flag, copy))

    send(z >= 1, direct(1, 5, y_to))
    send(odd, direct(2, 5, z_to_even))
    send(diag, direct(2, 5, z_to_odd))
    send(c1, direct(0, 5, x_near))
    send(c0 & high, direct(0, 5, x_far))
    send(relay_out, to_relay(2, 0, 3, side))
    send(diag & (x >= 2), to_relay(2, 1, 0, side))
    send(diag & (x >= 3), to_relay(2, 2, 1, side))
    send(c0 & high, to_relay(0, 1, 2, x_relay))
    send(c0 & (y == 3), to_relay(0, 2, 0, x_relay))
    send(c0 & (y == 3), to_relay(0, 3, 1, x_relay))
    for part in range(5):
        send(z >= 1, direct(1, part, y_to))
        send(odd, direct(2, part, z_to_even))
        send(c1, direct(0, part, x_near))
        if part == 1:
            send(diag & (x < 2), direct(2, part, z_to_odd))
        elif part == 2:
            send(diag & (x < 3), direct(2, part, z_to_odd))
        elif part > 2:
            send(diag, direct(2, part, z_to_odd))
        if part == 4:
            send(c0 & high, direct(0, part, x_far))
        elif part > 1:
            send(c0 & (y == 2), direct(0, part, x_far))

    forwarded = []

    def pass_on(flag, arrival, copies):
        @pl.when(flag)
        def _():
            arrival.wait_recv()
            for when, copy in copies:
                if when is None:
                    copy.start()
                else:
                    pl.when(when)(copy.start)

        for when, copy in copies:
            forwarded.append((flag if when is None else flag & when, copy))

    def x_relays():
        target = (x, 1 - y, z, 1)
        for part, slot in ((1, 2), (2, 0), (3, 1)):
            pass_on(
                (c0 & low) if part == 1 else (c0 & (y == 0)), to_relay(0, part, slot, x_relay),
                [(None, forward(0, part, relay_w.at[slot], slot, target))],
            )

    def interior_relay():
        pass_on(
            relay_in, to_relay(2, 0, 3, side),
            [
                (x >= 1, forward(2, 0, relay_a, 3, (x - 1, y, z, c))),
                (c0 & high, forward(0, 0, relay_a, 3, (x, y - 3, z, 1))),
            ],
        )

    def near_interior():
        pass_on(
            c0 & (y == 2), direct(2, 0, z_to_even),
            [(None, forward(0, 0, av.at[3], 3, (x, 1, z, 1)))],
        )

    def piece_relay(part):
        slot = part - 1
        pass_on(
            odd & (x >= part + 1), to_relay(2, part, slot, side),
            [(None, forward(2, part, relay_w.at[slot], slot, (x - 1, y, z, c)))],
        )

    def open_face(axis):
        return walls[axis] == 0

    def map_piece(w, a, m, n):
        piece = wv[w, :, cols(n)]
        mapped[m, :, cols(n)] = jnp.dot(
            av[a], piece, preferred_element_type=jnp.float32
        ).astype(jnp.bfloat16)
        turned[m, cols(n), :] = piece.T

    def upper(axis, carry):
        @pl.when(axis == 0)
        def _():
            loads[2].wait()

        pltpu.make_async_copy(wp_ref.at[axis], wv.at[axis], load_sem.at[axis]).wait()
        for n in range(PIECES):
            map_piece(axis, 0, axis, n)
        for n in range(PIECES):
            acc[axis, cols(n), :] = -jnp.dot(
                turned[axis, cols(n), :], mapped[axis], preferred_element_type=jnp.float32
            )
        return carry

    def edges(axis):
        band = step // 2
        is_open = open_face(axis)
        own = bpv[axis : axis + 1, :].astype(jnp.float32)
        other = bv[axis, axis : axis + 1, :].astype(jnp.float32)
        total = own + jnp.where(is_open, other, 0.0)
        link = jnp.where(is_open, -0.5, -0.25)

        def one(n, carry):
            shape = (band, width)
            p = lax.broadcasted_iota(jnp.int32, shape, 0) + n * band
            q = lax.broadcasted_iota(jnp.int32, shape, 1)
            apart = jnp.abs((p >> 5) - (q >> 5)) + jnp.abs((p & 31) - (q & 31))
            base = jnp.where(p == q, total, jnp.where(apart == 1, link, 0.0))
            rows = pl.ds(pl.multiple_of(n * band, band), band)
            acc[axis, rows, :] += base
            return carry

        lax.fori_loop(0, width // band, one, 0)

    def finish(axis, rows, columns, gram):
        total = acc[axis, rows, columns] - jnp.where(open_face(axis), gram, 0.0)
        out_ref[axis, rows, columns] = total.astype(jnp.bfloat16)

    def lower(axis, n):
        map_piece(3 + axis, 1 + axis, axis, n)
        seen = pl.ds(0, (n + 1) * step)
        finish(axis, cols(n), seen, jnp.dot(
            turned[axis, cols(n), :], mapped[axis, :, seen], preferred_element_type=jnp.float32
        ))
        if n:
            before = pl.ds(0, n * step)
            finish(axis, before, cols(n), jnp.dot(
                turned[axis, before, :], mapped[axis, :, cols(n)],
                preferred_element_type=jnp.float32,
            ))

    def arrived(axis, part):
        if part == 0:
            target = av.at[1 + axis]
        elif part == 5:
            target = bv.at[axis]
        else:
            target = wv.at[3 + axis, :, cols(part - 1)]
        source_ref = a_ref if part == 0 else bm_ref if part == 5 else wm_ref.at[axis, :, cols(part - 1)]
        pltpu.make_async_remote_copy(
            source_ref, target, send_sem.at[axis, part], recv_sem.at[axis, part],
            device_id=device_at(x, y, z, 1 - c), device_id_type=MESH,
        ).wait_recv()

    def wait_part(axis, part):
        if axis == 2 and part == 0:
            pl.when(has_z & jnp.logical_not(c0 & (y == 2)))(lambda: arrived(axis, part))
        else:
            pl.when((has_x, has_y, has_z)[axis])(lambda: arrived(axis, part))

    x_relays()
    lax.fori_loop(0, 3, upper, 0)
    near_interior()
    loads[0].wait()
    loads[1].wait()
    for axis in range(3):
        wait_part(axis, 5)
    for axis in range(3):
        edges(axis)

    @pl.when(c0)
    def _():
        arrived(0, 0)
        for n in range(PIECES):
            arrived(0, n + 1)
            lower(0, n)

    late_x = c1 & low

    def plain(axis, flag):
        @pl.when(flag)
        def _():
            out_ref[axis] = acc[axis].astype(jnp.bfloat16)

    plain(0, c1 & high)
    plain(1, jnp.logical_not(has_y))
    plain(2, jnp.logical_not(has_z))

    interior_relay()
    piece_relay(1)
    piece_relay(2)

    wait_part(1, 0)
    wait_part(2, 0)

    @pl.when(late_x)
    def _():
        arrived(0, 0)

    for n in range(PIECES):
        def one(t, carry, n=n):
            axis = (t + 1) % 3
            flag = ((axis == 0) & late_x) | ((axis == 1) & has_y) | ((axis == 2) & has_z)

            @pl.when(flag)
            def _():
                arrived(axis, n + 1)
                lower(axis, n)

            return carry

        lax.fori_loop(0, 3, one, 0)

    for flag, copy in sent + forwarded:
        pl.when(flag)(copy.wait_send)


def shards(w_minus, w_plus, interior, b_minus, b_plus, walls):
    rank, width = w_plus.shape[4:]
    faces = 3
    step = width // PIECES
    any_spec = pl.BlockSpec(memory_space=pltpu.HBM)
    out = pl.pallas_call(
        kernel,
        out_shape=pltpu.VMEM((faces, width, width), jnp.bfloat16),
        in_specs=[any_spec] * 6,
        out_specs=pl.BlockSpec(memory_space=pltpu.VMEM),
        scratch_shapes=[
            pltpu.VMEM((6, rank, width), jnp.bfloat16),
            pltpu.VMEM((4, rank, rank), jnp.bfloat16),
            pltpu.VMEM((3, faces, width), jnp.bfloat16),
            pltpu.VMEM((faces, width), jnp.bfloat16),
            pltpu.SMEM((faces,), jnp.int32),
            pltpu.VMEM((faces, width, width), jnp.float32),
            pltpu.VMEM((faces, rank, width), jnp.bfloat16),
            pltpu.VMEM((faces, width, rank), jnp.bfloat16),
            pltpu.VMEM((rank, rank), jnp.bfloat16),
            pltpu.VMEM((3, rank, step), jnp.bfloat16),
            pltpu.SemaphoreType.DMA((6,)),
            pltpu.SemaphoreType.DMA((3, 6)),
            pltpu.SemaphoreType.DMA((3, 6)),
            pltpu.SemaphoreType.DMA((3, 4)),
            pltpu.SemaphoreType.DMA((3, 4)),
            pltpu.SemaphoreType.DMA((3, 4)),
        ],
        compiler_params=pltpu.CompilerParams(
            collective_id=0, has_side_effects=True, vmem_limit_bytes=60000000
        ),
    )(
        w_minus[0, 0, 0], w_plus[0, 0, 0], interior[0, 0, 0], b_minus[0, 0, 0], b_plus[0, 0, 0],
        walls[0, 0, 0],
    )
    return out[None, None, None]


def solution(mesh):
    in_specs = (
        P("gx", "gy", "gz", None, None, None),
        P("gx", "gy", "gz", None, None, None),
        P("gx", "gy", "gz", None, None),
        P("gx", "gy", "gz", None, None),
        P("gx", "gy", "gz", None, None),
        P("gx", "gy", "gz", None),
    )
    out_specs = P("gx", "gy", "gz", None, None, None)
    return jax.shard_map(shards, mesh=mesh, in_specs=in_specs, out_specs=out_specs, check_vma=False)
```

```python
import jax
import jax.numpy as jnp
from jax import lax
from jax.experimental import pallas as pl
from jax.experimental.pallas import tpu as pltpu
from jax.sharding import PartitionSpec as P

FSIDE = 32
MESH = pl.DeviceIdType.MESH
PIECES = 4


def coordinates():
    gx, gy, gz = lax.axis_index("gx"), lax.axis_index("gy"), lax.axis_index("gz")
    return gz // 2, (gx // 2) * 2 + gz % 2, gy, gx % 2


def device_at(x, y, z, c):
    return ((y // 2) * 2 + c, z, x * 2 + y % 2)


def as_int(flag):
    return jnp.where(flag, 1, 0)


def kernel(
    wm_ref, wp_ref, a_ref, bm_ref, bp_ref, walls_ref, out_ref,
    wv, av, bv, bpv, walls, lows, acc, mapped, turned, relay_a, relay_w,
    load_sem, send_sem, recv_sem, relay_send, relay_recv, forward_send,
):
    x, y, z, c = coordinates()
    rank, width = wm_ref.shape[1], wm_ref.shape[2]
    step = width // PIECES
    odd = y % 2 == 1
    even = y % 2 == 0
    low, high = y < 2, y >= 2
    c0, c1 = c == 0, c == 1

    def cols(n):
        return pl.ds(n * step, step)

    to_send = [pltpu.make_async_copy(a_ref, av.at[0], load_sem.at[3])]
    for axis in (2, 0):
        to_send.append(pltpu.make_async_copy(wm_ref.at[axis], lows.at[axis], load_sem.at[6 + axis]))
    loads = [pltpu.make_async_copy(walls_ref, walls, load_sem.at[5])]
    loads.append(pltpu.make_async_copy(bp_ref, bpv, load_sem.at[4]))
    for axis in range(3):
        loads.append(pltpu.make_async_copy(wp_ref.at[axis], wv.at[axis], load_sem.at[axis]))
    for load in to_send + loads:
        load.start()

    has_y = z < 7
    has_z = jnp.logical_not(odd & (x == 3))
    has_x = c0 | low
    diag = even & (x >= 1)
    diag_in = odd & (x <= 2)
    relay_in = odd & ((x >= 1) | (c0 & high))
    relay_out = even & ((x >= 1) | (c0 & high))

    barrier = pltpu.get_barrier_semaphore()

    def greet(flag, *who):
        @pl.when(flag)
        def _():
            pl.semaphore_signal(barrier, inc=1, device_id=device_at(*who), device_id_type=MESH)

    greet(has_y, x, y, z + 1, c)
    greet(even, x, y + 1, z, c)
    greet(diag_in, x + 1, y - 1, z, c)
    greet(diag_in, x + 1, y, z, c)
    greet(relay_in, x, y - 1, z, c)
    greet(c0, x, y, z, 1)
    greet(c1 & low, x, y + 2, z, 0)
    greet(c1 & low, x, 1 - y, z, 0)
    greet(c1 & low, x, 3 - y, z, 0)
    greet(c0 & low, x, 3 - y, z, 0)

    partners = (
        as_int(z >= 1) + as_int(odd) + as_int(diag) + as_int(odd & (x >= 1)) + as_int(relay_out)
        + as_int(c1) + as_int(c0 & high) * 2 + as_int(c0)
    )
    pl.semaphore_wait(barrier, partners)

    half = rank // 2

    def halves(part):
        return pl.ds(part * half, half)

    def source(axis, part):
        if part < 2:
            return a_ref.at[halves(part)]
        if part == 6:
            return bm_ref
        if axis == 1:
            return wm_ref.at[axis, :, cols(part - 2)]
        return lows.at[axis, :, cols(part - 2)]

    def landing(axis, part):
        if part < 2:
            return av.at[1 + axis, halves(part)]
        if part == 6:
            return bv.at[axis]
        return wv.at[3 + axis, :, cols(part - 2)]

    def slot_ref(slot):
        return relay_a.at[halves(slot)] if slot < 2 else relay_w.at[slot - 2]

    def direct(axis, part, who):
        return pltpu.make_async_remote_copy(
            source(axis, part), landing(axis, part),
            send_sem.at[axis, part], recv_sem.at[axis, part],
            device_id=device_at(*who), device_id_type=MESH,
        )

    def to_relay(axis, part, slot, who):
        return pltpu.make_async_remote_copy(
            source(axis, part), slot_ref(slot),
            relay_send.at[axis, slot], relay_recv.at[axis, slot],
            device_id=device_at(*who), device_id_type=MESH,
        )

    def forward(axis, part, origin, slot, who):
        return pltpu.make_async_remote_copy(
            origin, landing(axis, part),
            forward_send.at[axis, slot], recv_sem.at[axis, part],
            device_id=device_at(*who), device_id_type=MESH,
        )

    y_to = (x, y, z - 1, c)
    z_to_even = (x, y - 1, z, c)
    z_to_odd = (x - 1, y + 1, z, c)
    side = (x, y + 1, z, c)
    x_near = (x, y, z, 0)
    x_far = (x, y - 2, z, 1)
    x_relay = (x, 3 - y, z, 0)

    sent = []

    def send(flag, copy):
        @pl.when(flag)
        def _():
            copy.start()

        sent.append((flag, copy))

    send(z >= 1, direct(1, 6, y_to))
    send(odd, direct(2, 6, z_to_even))
    send(diag, direct(2, 6, z_to_odd))
    send(c1, direct(0, 6, x_near))
    send(c0 & high, direct(0, 6, x_far))
    def goes_round(part):
        return x + c >= part

    diagonal_relayed = [
        (relay_out, to_relay(2, 0, 0, side)),
        (relay_out, to_relay(2, 1, 1, side)),
        (diag & goes_round(2), to_relay(2, 2, 2, side)),
        (diag & goes_round(3), to_relay(2, 3, 3, side)),
        (diag & goes_round(4), to_relay(2, 4, 4, side)),
    ]
    for flag, copy in diagonal_relayed[:2]:
        pl.when(flag)(copy.start)
    for part in range(2):
        send(odd, direct(2, part, z_to_even))
    for part in range(6):
        send(z >= 1, direct(1, part, y_to))
    for load in to_send:
        load.wait()
    for flag, copy in diagonal_relayed[2:]:
        pl.when(flag)(copy.start)
    send(c0 & high, to_relay(0, 2, 5, x_relay))
    send(c0 & (y == 3), to_relay(0, 3, 2, x_relay))
    send(c0 & (y == 3), to_relay(0, 4, 3, x_relay))
    send(c0 & (y == 3), direct(0, 5, x_far))
    corner = c0 & (x == 0)
    for part in (3, 4, 5):
        send(c0 & (y == 2) & (x >= 1), direct(0, part, x_far))
        send(corner & (y == 2), to_relay(0, part, part - 1, side))
    keeps = c0 & (y == 1)
    for part in range(2, 6):
        send(odd & jnp.logical_not(keeps) if part > 3 else odd, direct(2, part, z_to_even))
    for part in range(6):
        send(c1, direct(0, part, x_near))
    straight = [
        (diag & jnp.logical_not(goes_round(part)), direct(2, part, z_to_odd)) for part in range(2, 5)
    ] + [(diag, direct(2, 5, z_to_odd))]
    sent.extend(straight)

    def send_diagonal(now):
        for flag, copy in diagonal_relayed:
            pl.when(flag & now)(copy.wait_send)
        for flag, copy in straight:
            pl.when(flag & now)(copy.start)

    forwarded = []

    def pass_on(flag, arrival, copies):
        @pl.when(flag)
        def _():
            arrival.wait_recv()
            for when, copy in copies:
                if when is None:
                    copy.start()
                else:
                    pl.when(when)(copy.start)

        for when, copy in copies:
            forwarded.append((flag if when is None else flag & when, copy))

    x_relayed = ((c0 & low, 2, 5), (c0 & (y == 0), 3, 2), (c0 & (y == 0), 4, 3))

    def x_forward(part, slot):
        return forward(0, part, slot_ref(slot), slot, (x, 1 - y, z, 1))

    def x_relay_piece(n, when):
        flag, part, slot = x_relayed[n]

        @pl.when(flag & when)
        def _():
            to_relay(0, part, slot, x_relay).wait_recv()
            x_forward(part, slot).start()

    for flag, part, slot in x_relayed:
        forwarded.append((flag, x_forward(part, slot)))

    def interior_relay(part):
        pass_on(
            relay_in, to_relay(2, part, part, side),
            [
                (x >= 1, forward(2, part, slot_ref(part), part, (x - 1, y, z, c))),
                (c0 & high, forward(0, part, slot_ref(part), part, (x, y - 3, z, 1))),
            ],
        )

    def corner_relay():
        for part in (3, 4, 5):
            slot = part - 1
            pass_on(
                corner & (y == 3), to_relay(0, part, slot, side),
                [(None, forward(0, part, slot_ref(slot), slot, (x, 0, z, 1)))],
            )

    def near_interior():
        for part in range(2):
            pass_on(
                c0 & (y == 2), direct(2, part, z_to_even),
                [(None, forward(0, part, av.at[3, halves(part)], part, (x, 1, z, 1)))],
            )

    def piece_relay(part):
        pass_on(
            odd & goes_round(part), to_relay(2, part, part, side),
            [(None, forward(2, part, slot_ref(part), part, (x - 1, y, z, c)))],
        )

    def open_face(axis):
        return walls[axis] == 0

    def map_piece(w, a, m, n):
        piece = wv[w, :, cols(n)]
        mapped[m, :, cols(n)] = jnp.dot(
            av[a], piece, preferred_element_type=jnp.float32
        ).astype(jnp.bfloat16)
        turned[m, cols(n), :] = piece.T

    def upper(axis, carry):

        pltpu.make_async_copy(wp_ref.at[axis], wv.at[axis], load_sem.at[axis]).wait()
        for n in range(PIECES):
            map_piece(axis, 0, axis, n)
        for n in range(PIECES):
            acc[axis, cols(n), :] = -jnp.dot(
                turned[axis, cols(n), :], mapped[axis], preferred_element_type=jnp.float32
            )
        return carry

    def edges(axis):
        band = step // 2
        is_open = open_face(axis)
        own = bpv[axis : axis + 1, :].astype(jnp.float32)
        other = bv[axis, axis : axis + 1, :].astype(jnp.float32)
        total = own + jnp.where(is_open, other, 0.0)
        link = jnp.where(is_open, -0.5, -0.25)

        def one(n, carry):
            shape = (band, width)
            p = lax.broadcasted_iota(jnp.int32, shape, 0) + n * band
            q = lax.broadcasted_iota(jnp.int32, shape, 1)
            apart = jnp.abs((p >> 5) - (q >> 5)) + jnp.abs((p & 31) - (q & 31))
            base = jnp.where(p == q, total, jnp.where(apart == 1, link, 0.0))
            rows = pl.ds(pl.multiple_of(n * band, band), band)
            acc[axis, rows, :] += base
            return carry

        lax.fori_loop(0, width // band, one, 0)

    def finish(axis, rows, columns, gram):
        total = acc[axis, rows, columns] - jnp.where(open_face(axis), gram, 0.0)
        out_ref[axis, rows, columns] = total.astype(jnp.bfloat16)

    def lower(axis, n):
        map_piece(3 + axis, 1 + axis, axis, n)
        seen = pl.ds(0, (n + 1) * step)
        finish(axis, cols(n), seen, jnp.dot(
            turned[axis, cols(n), :], mapped[axis, :, seen], preferred_element_type=jnp.float32
        ))
        if n:
            before = pl.ds(0, n * step)
            finish(axis, before, cols(n), jnp.dot(
                turned[axis, before, :], mapped[axis, :, cols(n)],
                preferred_element_type=jnp.float32,
            ))

    def arrived(axis, part):
        pltpu.make_async_remote_copy(
            landing(axis, part), landing(axis, part),
            send_sem.at[axis, part], recv_sem.at[axis, part],
            device_id=device_at(x, y, z, 1 - c), device_id_type=MESH,
        ).wait_recv()

    def wait_part(axis, part):
        if axis == 2 and part < 2:
            pl.when(has_z & jnp.logical_not(c0 & (y == 2)))(lambda: arrived(axis, part))
        else:
            pl.when((has_x, has_y, has_z)[axis])(lambda: arrived(axis, part))

    for n in range(2):
        x_relay_piece(n, True)
    for part in (4, 5):
        send(keeps, direct(2, part, z_to_even))
    x_relay_piece(2, x == 0)
    lax.fori_loop(0, 3, upper, 0)
    x_relay_piece(2, x >= 1)
    send_diagonal(c0 & (x <= 1) & (y == 0))
    interior_relay(0)
    near_interior()
    loads[0].wait()
    loads[1].wait()
    for axis in range(3):
        wait_part(axis, 6)
    edges(0)
    edges(1)
    interior_relay(1)
    edges(2)
    send_diagonal((x <= 1) & c1)
    send_diagonal((x == 2) & c0 & (y == 0))

    @pl.when(c0)
    def _():
        arrived(0, 0)
        arrived(0, 1)
        for n in range(PIECES):
            arrived(0, n + 2)
            lower(0, n)

    send_diagonal((x <= 1) & c0 & (y > 0))
    corner_relay()
    late_x = c1 & low

    def plain(axis, flag):
        @pl.when(flag)
        def _():
            out_ref[axis] = acc[axis].astype(jnp.bfloat16)

    piece_relay(2)
    plain(0, c1 & high)
    plain(1, jnp.logical_not(has_y))
    plain(2, jnp.logical_not(has_z))
    piece_relay(3)
    send_diagonal((x == 2) & (c1 | (y > 0)))

    for part in range(2):
        wait_part(1, part)
        wait_part(2, part)

    def y_and_z(n):
        def one(t, carry):
            axis = t + 1

            @pl.when(((axis == 1) & has_y) | ((axis == 2) & has_z))
            def _():
                arrived(axis, n + 2)
                lower(axis, n)

            return carry

        lax.fori_loop(0, 2, one, 0)

    y_and_z(0)
    y_and_z(1)

    def x_late(*pieces):
        @pl.when(late_x)
        def _():
            for n in pieces:
                arrived(0, n + 2)
                lower(0, n)

    for part in range(2):
        pl.when(late_x)(lambda part=part: arrived(0, part))
    x_late(0)
    piece_relay(4)
    send_diagonal(x == 3)
    x_late(1)
    y_and_z(2)
    x_late(2)
    y_and_z(3)
    x_late(3)

    for flag, copy in sent + forwarded:
        pl.when(flag)(copy.wait_send)


def shards(w_minus, w_plus, interior, b_minus, b_plus, walls):
    rank, width = w_plus.shape[4:]
    faces = 3
    step = width // PIECES
    any_spec = pl.BlockSpec(memory_space=pltpu.HBM)
    out = pl.pallas_call(
        kernel,
        out_shape=pltpu.VMEM((faces, width, width), jnp.bfloat16),
        in_specs=[any_spec] * 6,
        out_specs=pl.BlockSpec(memory_space=pltpu.VMEM),
        scratch_shapes=[
            pltpu.VMEM((6, rank, width), jnp.bfloat16),
            pltpu.VMEM((4, rank, rank), jnp.bfloat16),
            pltpu.VMEM((3, faces, width), jnp.bfloat16),
            pltpu.VMEM((faces, width), jnp.bfloat16),
            pltpu.SMEM((faces,), jnp.int32),
            pltpu.VMEM((faces, rank, width), jnp.bfloat16),
            pltpu.VMEM((faces, width, width), jnp.float32),
            pltpu.VMEM((faces, rank, width), jnp.bfloat16),
            pltpu.VMEM((faces, width, rank), jnp.bfloat16),
            pltpu.VMEM((rank, rank), jnp.bfloat16),
            pltpu.VMEM((PIECES, rank, step), jnp.bfloat16),
            pltpu.SemaphoreType.DMA((9,)),
            pltpu.SemaphoreType.DMA((3, 7)),
            pltpu.SemaphoreType.DMA((3, 7)),
            pltpu.SemaphoreType.DMA((3, 6)),
            pltpu.SemaphoreType.DMA((3, 6)),
            pltpu.SemaphoreType.DMA((3, 6)),
        ],
        compiler_params=pltpu.CompilerParams(
            collective_id=0, has_side_effects=True, vmem_limit_bytes=60000000
        ),
    )(
        w_minus[0, 0, 0], w_plus[0, 0, 0], interior[0, 0, 0], b_minus[0, 0, 0], b_plus[0, 0, 0],
        walls[0, 0, 0],
    )
    return out[None, None, None]


def solution(mesh):
    in_specs = (
        P("gx", "gy", "gz", None, None, None),
        P("gx", "gy", "gz", None, None, None),
        P("gx", "gy", "gz", None, None),
        P("gx", "gy", "gz", None, None),
        P("gx", "gy", "gz", None, None),
        P("gx", "gy", "gz", None),
    )
    out_specs = P("gx", "gy", "gz", None, None, None)
    return jax.shard_map(shards, mesh=mesh, in_specs=in_specs, out_specs=out_specs, check_vma=False)
```

```python
import jax
import jax.numpy as jnp
from jax import lax
from jax.experimental import pallas as pl
from jax.experimental.pallas import tpu as pltpu
from jax.sharding import PartitionSpec as P

FSIDE = 32
MESH = pl.DeviceIdType.MESH
PIECES = 4


def coordinates():
    gx, gy, gz = lax.axis_index("gx"), lax.axis_index("gy"), lax.axis_index("gz")
    return gz // 2, (gx // 2) * 2 + gz % 2, gy, gx % 2


def device_at(x, y, z, c):
    return ((y // 2) * 2 + c, z, x * 2 + y % 2)


def as_int(flag):
    return jnp.where(flag, 1, 0)


def kernel(
    wm_ref, wp_ref, a_ref, bm_ref, bp_ref, walls_ref, out_ref,
    wv, av, bv, bpv, walls, lows, acc, mapped, turned, relay_a, relay_w,
    load_sem, send_sem, recv_sem, relay_send, relay_recv, forward_send,
):
    x, y, z, c = coordinates()
    rank, width = wm_ref.shape[1], wm_ref.shape[2]
    step = width // PIECES
    odd = y % 2 == 1
    even = y % 2 == 0
    low, high = y < 2, y >= 2
    c0, c1 = c == 0, c == 1

    def cols(n):
        return pl.ds(n * step, step)

    to_send = [pltpu.make_async_copy(a_ref, av.at[0], load_sem.at[3])]
    for axis in (2, 0):
        to_send.append(pltpu.make_async_copy(wm_ref.at[axis], lows.at[axis], load_sem.at[6 + axis]))
    loads = [pltpu.make_async_copy(walls_ref, walls, load_sem.at[5])]
    loads.append(pltpu.make_async_copy(bp_ref, bpv, load_sem.at[4]))
    for axis in range(3):
        loads.append(pltpu.make_async_copy(wp_ref.at[axis], wv.at[axis], load_sem.at[axis]))
    for load in to_send + loads:
        load.start()

    has_y = z < 7
    has_z = jnp.logical_not(odd & (x == 3))
    has_x = c0 | low
    diag = even & (x >= 1)
    diag_in = odd & (x <= 2)
    relay_in = odd & ((x >= 1) | (c0 & high))
    relay_out = even & ((x >= 1) | (c0 & high))

    barrier = pltpu.get_barrier_semaphore()

    def greet(flag, *who):
        @pl.when(flag)
        def _():
            pl.semaphore_signal(barrier, inc=1, device_id=device_at(*who), device_id_type=MESH)

    greet(has_y, x, y, z + 1, c)
    greet(even, x, y + 1, z, c)
    greet(diag_in, x + 1, y - 1, z, c)
    greet(diag_in, x + 1, y, z, c)
    greet(relay_in, x, y - 1, z, c)
    greet(c0, x, y, z, 1)
    greet(c1 & low, x, y + 2, z, 0)
    greet(c1 & low, x, 1 - y, z, 0)
    greet(c1 & low, x, 3 - y, z, 0)
    greet(c0 & low, x, 3 - y, z, 0)

    partners = (
        as_int(z >= 1) + as_int(odd) + as_int(diag) + as_int(odd & (x >= 1)) + as_int(relay_out)
        + as_int(c1) + as_int(c0 & high) * 2 + as_int(c0)
    )
    pl.semaphore_wait(barrier, partners)

    half = rank // 2

    def halves(part):
        return pl.ds(part * half, half)

    def source(axis, part):
        if part < 2:
            return a_ref.at[halves(part)]
        if part == 6:
            return bm_ref
        if axis == 1:
            return wm_ref.at[axis, :, cols(part - 2)]
        return lows.at[axis, :, cols(part - 2)]

    def landing(axis, part):
        if part < 2:
            return av.at[1 + axis, halves(part)]
        if part == 6:
            return bv.at[axis]
        return wv.at[3 + axis, :, cols(part - 2)]

    def slot_ref(slot):
        return relay_a.at[halves(slot)] if slot < 2 else relay_w.at[slot - 2]

    def direct(axis, part, who):
        return pltpu.make_async_remote_copy(
            source(axis, part), landing(axis, part),
            send_sem.at[axis, part], recv_sem.at[axis, part],
            device_id=device_at(*who), device_id_type=MESH,
        )

    def to_relay(axis, part, slot, who):
        return pltpu.make_async_remote_copy(
            source(axis, part), slot_ref(slot),
            relay_send.at[axis, slot], relay_recv.at[axis, slot],
            device_id=device_at(*who), device_id_type=MESH,
        )

    def forward(axis, part, origin, slot, who):
        return pltpu.make_async_remote_copy(
            origin, landing(axis, part),
            forward_send.at[axis, slot], recv_sem.at[axis, part],
            device_id=device_at(*who), device_id_type=MESH,
        )

    y_to = (x, y, z - 1, c)
    z_to_even = (x, y - 1, z, c)
    z_to_odd = (x - 1, y + 1, z, c)
    side = (x, y + 1, z, c)
    x_near = (x, y, z, 0)
    x_far = (x, y - 2, z, 1)
    x_relay = (x, 3 - y, z, 0)

    sent = []

    def send(flag, copy):
        @pl.when(flag)
        def _():
            copy.start()

        sent.append((flag, copy))

    send(z >= 1, direct(1, 6, y_to))
    send(odd, direct(2, 6, z_to_even))
    send(diag, direct(2, 6, z_to_odd))
    send(c1, direct(0, 6, x_near))
    send(c0 & high, direct(0, 6, x_far))
    def goes_round(part):
        return ((x != 2) & (x + c >= part)) | ((x == 2) & c1 & (part < 5))

    diagonal_relayed = [
        (relay_out, to_relay(2, 0, 0, side)),
        (relay_out, to_relay(2, 1, 1, side)),
        (diag & goes_round(2), to_relay(2, 2, 2, side)),
        (diag & goes_round(3), to_relay(2, 3, 3, side)),
        (diag & goes_round(4), to_relay(2, 4, 4, side)),
    ]
    for flag, copy in diagonal_relayed[:2]:
        pl.when(flag)(copy.start)
    for part in range(2):
        send(odd, direct(2, part, z_to_even))
    for part in range(6):
        send(z >= 1, direct(1, part, y_to))
    for load in to_send:
        load.wait()
    for flag, copy in diagonal_relayed[2:]:
        pl.when(flag)(copy.start)
    send(c0 & high, to_relay(0, 2, 5, x_relay))
    send(c0 & (y == 3), to_relay(0, 3, 2, x_relay))
    send(c0 & (y == 3), to_relay(0, 4, 3, x_relay))
    send(c0 & (y == 3), direct(0, 5, x_far))
    corner = c0 & (x == 0)
    for part in (3, 4, 5):
        send(c0 & (y == 2) & (x >= 1), direct(0, part, x_far))
        send(corner & (y == 2), to_relay(0, part, part - 1, side))
    keeps = c0 & (y == 1)
    for part in range(2, 6):
        send(odd & jnp.logical_not(keeps) if part > 3 else odd, direct(2, part, z_to_even))
    for part in range(6):
        send(c1, direct(0, part, x_near))
    straight = [
        (diag & jnp.logical_not(goes_round(part)), direct(2, part, z_to_odd)) for part in range(2, 5)
    ] + [(diag, direct(2, 5, z_to_odd))]
    sent.extend(straight)

    def send_diagonal(now):
        for flag, copy in diagonal_relayed:
            pl.when(flag & now)(copy.wait_send)
        for flag, copy in straight:
            pl.when(flag & now)(copy.start)

    forwarded = []

    def pass_on(flag, arrival, copies):
        @pl.when(flag)
        def _():
            arrival.wait_recv()
            for when, copy in copies:
                if when is None:
                    copy.start()
                else:
                    pl.when(when)(copy.start)

        for when, copy in copies:
            forwarded.append((flag if when is None else flag & when, copy))

    x_relayed = ((c0 & low, 2, 5), (c0 & (y == 0), 3, 2), (c0 & (y == 0), 4, 3))

    def x_forward(part, slot):
        return forward(0, part, slot_ref(slot), slot, (x, 1 - y, z, 1))

    def x_relay_piece(n, when):
        flag, part, slot = x_relayed[n]

        @pl.when(flag & when)
        def _():
            to_relay(0, part, slot, x_relay).wait_recv()
            x_forward(part, slot).start()

    for flag, part, slot in x_relayed:
        forwarded.append((flag, x_forward(part, slot)))

    def interior_relay(part):
        pass_on(
            relay_in, to_relay(2, part, part, side),
            [
                (x >= 1, forward(2, part, slot_ref(part), part, (x - 1, y, z, c))),
                (c0 & high, forward(0, part, slot_ref(part), part, (x, y - 3, z, 1))),
            ],
        )

    def corner_relay():
        for part in (3, 4, 5):
            slot = part - 1
            pass_on(
                corner & (y == 3), to_relay(0, part, slot, side),
                [(None, forward(0, part, slot_ref(slot), slot, (x, 0, z, 1)))],
            )

    def near_interior():
        for part in range(2):
            pass_on(
                c0 & (y == 2), direct(2, part, z_to_even),
                [(None, forward(0, part, av.at[3, halves(part)], part, (x, 1, z, 1)))],
            )

    def piece_relay(part):
        pass_on(
            odd & goes_round(part), to_relay(2, part, part, side),
            [(None, forward(2, part, slot_ref(part), part, (x - 1, y, z, c)))],
        )

    def open_face(axis):
        return walls[axis] == 0

    def map_piece(w, a, m, n):
        piece = wv[w, :, cols(n)]
        mapped[m, :, cols(n)] = jnp.dot(
            av[a], piece, preferred_element_type=jnp.float32
        ).astype(jnp.bfloat16)
        turned[m, cols(n), :] = piece.T

    def upper(axis, carry):

        pltpu.make_async_copy(wp_ref.at[axis], wv.at[axis], load_sem.at[axis]).wait()
        for n in range(PIECES):
            map_piece(axis, 0, axis, n)
        for n in range(PIECES):
            acc[axis, cols(n), :] = -jnp.dot(
                turned[axis, cols(n), :], mapped[axis], preferred_element_type=jnp.float32
            )
        return carry

    def edges(axis):
        band = step // 2
        is_open = open_face(axis)
        own = bpv[axis : axis + 1, :].astype(jnp.float32)
        other = bv[axis, axis : axis + 1, :].astype(jnp.float32)
        total = own + jnp.where(is_open, other, 0.0)
        link = jnp.where(is_open, -0.5, -0.25)

        def one(n, carry):
            shape = (band, width)
            p = lax.broadcasted_iota(jnp.int32, shape, 0) + n * band
            q = lax.broadcasted_iota(jnp.int32, shape, 1)
            apart = jnp.abs((p >> 5) - (q >> 5)) + jnp.abs((p & 31) - (q & 31))
            base = jnp.where(p == q, total, jnp.where(apart == 1, link, 0.0))
            rows = pl.ds(pl.multiple_of(n * band, band), band)
            acc[axis, rows, :] += base
            return carry

        lax.fori_loop(0, width // band, one, 0)

    def finish(axis, rows, columns, gram):
        total = acc[axis, rows, columns] - jnp.where(open_face(axis), gram, 0.0)
        out_ref[axis, rows, columns] = total.astype(jnp.bfloat16)

    def lower(axis, n):
        map_piece(3 + axis, 1 + axis, axis, n)
        seen = pl.ds(0, (n + 1) * step)
        finish(axis, cols(n), seen, jnp.dot(
            turned[axis, cols(n), :], mapped[axis, :, seen], preferred_element_type=jnp.float32
        ))
        if n:
            before = pl.ds(0, n * step)
            finish(axis, before, cols(n), jnp.dot(
                turned[axis, before, :], mapped[axis, :, cols(n)],
                preferred_element_type=jnp.float32,
            ))

    def arrived(axis, part):
        pltpu.make_async_remote_copy(
            landing(axis, part), landing(axis, part),
            send_sem.at[axis, part], recv_sem.at[axis, part],
            device_id=device_at(x, y, z, 1 - c), device_id_type=MESH,
        ).wait_recv()

    def wait_part(axis, part):
        if axis == 2 and part < 2:
            pl.when(has_z & jnp.logical_not(c0 & (y == 2)))(lambda: arrived(axis, part))
        else:
            pl.when((has_x, has_y, has_z)[axis])(lambda: arrived(axis, part))

    for n in range(2):
        x_relay_piece(n, True)
    for part in (4, 5):
        send(keeps, direct(2, part, z_to_even))
    x_relay_piece(2, x == 0)
    lax.fori_loop(0, 3, upper, 0)
    x_relay_piece(2, x >= 1)
    send_diagonal(c0 & (x <= 1) & (y == 0))
    interior_relay(0)
    near_interior()
    loads[0].wait()
    loads[1].wait()
    for axis in range(3):
        wait_part(axis, 6)
    edges(0)
    edges(1)
    interior_relay(1)
    edges(2)
    send_diagonal((x <= 1) & c1)
    send_diagonal((x == 2) & c0 & (y == 0))

    @pl.when(c0)
    def _():
        arrived(0, 0)
        arrived(0, 1)
        for n in range(PIECES):
            arrived(0, n + 2)
            lower(0, n)

    send_diagonal((x <= 1) & c0 & (y > 0))
    corner_relay()
    late_x = c1 & low

    def plain(axis, flag):
        @pl.when(flag)
        def _():
            out_ref[axis] = acc[axis].astype(jnp.bfloat16)

    piece_relay(2)
    plain(0, c1 & high)
    plain(1, jnp.logical_not(has_y))
    plain(2, jnp.logical_not(has_z))
    piece_relay(3)
    send_diagonal((x == 2) & (c1 | (y > 0)))

    for part in range(2):
        wait_part(1, part)
        wait_part(2, part)

    def y_and_z(n):
        def one(t, carry):
            axis = t + 1

            @pl.when(((axis == 1) & has_y) | ((axis == 2) & has_z))
            def _():
                arrived(axis, n + 2)
                lower(axis, n)

            return carry

        lax.fori_loop(0, 2, one, 0)

    y_and_z(0)
    early = (x == 3) & c0 & (y == 2)
    for flag, copy in diagonal_relayed:
        pl.when(flag & early)(copy.wait_send)
    pl.when(early)(straight[2][1].start)
    y_and_z(1)

    def x_late(*pieces):
        @pl.when(late_x)
        def _():
            for n in pieces:
                arrived(0, n + 2)
                lower(0, n)

    for part in range(2):
        pl.when(late_x)(lambda part=part: arrived(0, part))
    x_late(0)
    piece_relay(4)
    send_diagonal((x == 3) & jnp.logical_not(early))
    pl.when(early)(straight[3][1].start)
    x_late(1)
    y_and_z(2)
    x_late(2)
    y_and_z(3)
    x_late(3)

    for flag, copy in sent + forwarded:
        pl.when(flag)(copy.wait_send)


def shards(w_minus, w_plus, interior, b_minus, b_plus, walls):
    rank, width = w_plus.shape[4:]
    faces = 3
    step = width // PIECES
    any_spec = pl.BlockSpec(memory_space=pltpu.HBM)
    out = pl.pallas_call(
        kernel,
        out_shape=pltpu.VMEM((faces, width, width), jnp.bfloat16),
        in_specs=[any_spec] * 6,
        out_specs=pl.BlockSpec(memory_space=pltpu.VMEM),
        scratch_shapes=[
            pltpu.VMEM((6, rank, width), jnp.bfloat16),
            pltpu.VMEM((4, rank, rank), jnp.bfloat16),
            pltpu.VMEM((3, faces, width), jnp.bfloat16),
            pltpu.VMEM((faces, width), jnp.bfloat16),
            pltpu.SMEM((faces,), jnp.int32),
            pltpu.VMEM((faces, rank, width), jnp.bfloat16),
            pltpu.VMEM((faces, width, width), jnp.float32),
            pltpu.VMEM((faces, rank, width), jnp.bfloat16),
            pltpu.VMEM((faces, width, rank), jnp.bfloat16),
            pltpu.VMEM((rank, rank), jnp.bfloat16),
            pltpu.VMEM((PIECES, rank, step), jnp.bfloat16),
            pltpu.SemaphoreType.DMA((9,)),
            pltpu.SemaphoreType.DMA((3, 7)),
            pltpu.SemaphoreType.DMA((3, 7)),
            pltpu.SemaphoreType.DMA((3, 6)),
            pltpu.SemaphoreType.DMA((3, 6)),
            pltpu.SemaphoreType.DMA((3, 6)),
        ],
        compiler_params=pltpu.CompilerParams(
            collective_id=0, has_side_effects=True, vmem_limit_bytes=60000000
        ),
    )(
        w_minus[0, 0, 0], w_plus[0, 0, 0], interior[0, 0, 0], b_minus[0, 0, 0], b_plus[0, 0, 0],
        walls[0, 0, 0],
    )
    return out[None, None, None]


def solution(mesh):
    in_specs = (
        P("gx", "gy", "gz", None, None, None),
        P("gx", "gy", "gz", None, None, None),
        P("gx", "gy", "gz", None, None),
        P("gx", "gy", "gz", None, None),
        P("gx", "gy", "gz", None, None),
        P("gx", "gy", "gz", None),
    )
    out_specs = P("gx", "gy", "gz", None, None, None)
    return jax.shard_map(shards, mesh=mesh, in_specs=in_specs, out_specs=out_specs, check_vma=False)
```
